32 devices in a mesh: len: 2 (over x), tile: 16 (over z, y, core).
Axes of the slice: x: 2, y: 2, z: 4, core: 2. Of those that a mesh axis runs over, the one named last changes fastest.
Arguments:
- series: float32 [9216], P('tile'), may hold values from -24 to 24
- window_lengths: int32 [4], P('len'), may hold values from 64 to 1024, as said below
- exclusion: int32 [4], P('len'), may hold values from 16 to 256
- tile_list: int32 [64, 2], P('tile'), may hold values from 0 to 15, as said below
Outputs:
- right_profile: float32 [4, 8192], P(None, 'tile')
- left_profile: float32 [4, 8192], P(None, 'tile')
The draws below stay inside these ranges and needn't reach their ends.
Inputs may be any that keep to these rules, and one draw needn't show every extreme that they name: `window_lengths`: the largest is exactly 1024. `tile_list`: each row is a pair (row block, column block) with row block <= column block; no pair appears twice.
All inputs are finite; a program needn't handle non-finite values.
Results may differ from the reference program's by a relative error of at most 0.00039.
Values sent between devices are 32-bit elements; how exact they have to be, the bound alone decides.
A program may use at most 64 MiB of HBM per device.

```python
import jax
import jax.numpy as jnp
from jax import lax

MIN_LEN = 64
OCTAVES = 4
MAX_LEN = 1024
LENGTHS = 4
TILE_SIDE = 512
COL_BLOCK = 512
TILE_ROWS = 16
SERIES_LENGTH = 9216
TILE_SLOTS = 64


def draw_series(key, part):
    noise_key, wave_key, phase_key = jax.random.split(key, 3)
    sample_times = jnp.arange(SERIES_LENGTH, dtype=jnp.float32)
    wave_frequencies = jax.random.uniform(wave_key, (4,), jnp.float32, 0.002, 0.05)
    wave_phases = jax.random.uniform(phase_key, (4,), jnp.float32, -3.14159, 3.14159)
    smoothed_series = 0.5 * jnp.sum(jnp.sin(sample_times[:, None] * wave_frequencies[None, :] + wave_phases[None, :]), axis=1)
    jitter = jnp.clip(jax.random.normal(noise_key, (SERIES_LENGTH,), jnp.float32), -6.0, 6.0)
    return jitter + smoothed_series


def draw_window_lengths(key, part):
    octave_key, offset_key, pick_key = jax.random.split(key, 3)
    octave = jax.random.randint(octave_key, (LENGTHS,), 0, OCTAVES)
    lowest = MIN_LEN * jnp.left_shift(jnp.ones((LENGTHS,), jnp.int32), octave.astype(jnp.int32))
    surplus = jax.random.randint(offset_key, (LENGTHS,), 0, 1 << 30) % (lowest + 1)
    chosen = jax.random.randint(pick_key, (), 0, LENGTHS)
    lengths = jnp.where(jnp.arange(LENGTHS) == chosen, MAX_LEN, lowest + surplus)
    return lengths.astype(jnp.int32)


def draw_tile_list(key, part):
    grid_rows = lax.broadcasted_iota(jnp.int32, (TILE_ROWS, TILE_ROWS), 0)
    grid_cols = lax.broadcasted_iota(jnp.int32, (TILE_ROWS, TILE_ROWS), 1)
    upper = (grid_rows <= grid_cols).reshape(-1)
    triangle = TILE_ROWS * (TILE_ROWS + 1) // 2
    flat_ids = jnp.nonzero(upper, size=triangle)[0].astype(jnp.int32)
    order = jax.random.permutation(key, triangle)[:TILE_SLOTS]
    picked = flat_ids[order]
    return jnp.stack([picked // TILE_ROWS, picked % TILE_ROWS], axis=1).astype(jnp.int32)


def place_ends(result, stream_key, low, largest):
    spot = [jax.random.randint(jax.random.fold_in(stream_key, axis), (), 0, length) for axis, length in enumerate(result.shape)]
    longest = result.shape.index(max(result.shape))
    neighbour = spot[:longest] + [(spot[longest] + 1) % result.shape[longest]] + spot[longest + 1:]
    return result.at[tuple(spot)].set(low).at[tuple(neighbour)].set(largest)


def setup_inputs(seed: int = 0) -> dict:
    keys = jax.random.split(jax.random.key(seed), 5)
    series = draw_series(jax.random.fold_in(keys[4], 71), 0)
    window_lengths = draw_window_lengths(jax.random.fold_in(keys[4], 71), 0)
    exclusion = place_ends(jax.random.randint(keys[2], (LENGTHS,), MIN_LEN // 4, MAX_LEN // 4 + 1), jax.random.fold_in(keys[2], 1), MIN_LEN // 4, (MAX_LEN // 4 + 1) - 1).astype(jnp.int32)
    tile_list = draw_tile_list(jax.random.fold_in(keys[4], 71), 0)
    return {"series": series, "window_lengths": window_lengths, "exclusion": exclusion, "tile_list": tile_list}


EMPTY_VALUE = 2.0
VAR_EPS = 1e-05

def shifted_block(segment, offset, columns, positions):
    window = lax.dynamic_slice_in_dim(segment, offset, positions + columns)
    stride = positions + columns + 1
    repeated = jnp.tile(window, columns + 1)[:columns * stride]
    return repeated.reshape(columns, stride)[:, :positions]

def window_stats(segment, length, positions, columns):
    blocks = (length + columns - 1) // columns
    col_ids = lax.broadcasted_iota(jnp.int32, (columns, 1), 0)
    denominator = length.astype(jnp.float32)
    initial = jnp.zeros((positions,), jnp.float32)

    def add_sum(part_index, running):
        values = shifted_block(segment, part_index * columns, columns, positions)
        inside = col_ids + part_index * columns < length
        return running + lax.optimization_barrier(jnp.sum(jnp.where(inside, values, 0.0), axis=0))
    centre = lax.fori_loop(0, blocks, add_sum, initial) / denominator

    def add_square(part_index, running):
        values = shifted_block(segment, part_index * columns, columns, positions) - centre[None, :]
        inside = col_ids + part_index * columns < length
        return running + lax.optimization_barrier(jnp.sum(jnp.where(inside, values * values, 0.0), axis=0))
    spread = lax.fori_loop(0, blocks, add_square, initial) / denominator
    return (centre, 1.0 / jnp.sqrt(spread + VAR_EPS))

def normalized(segment, part_index, centre, inverse, length):
    values = shifted_block(segment, part_index * COL_BLOCK, COL_BLOCK, TILE_SIDE)
    col_ids = lax.broadcasted_iota(jnp.int32, (COL_BLOCK, 1), 0)
    inside = col_ids + part_index * COL_BLOCK < length
    return jnp.where(inside, (values - centre[None, :]) * inverse[None, :], 0.0).astype(jnp.bfloat16)

def tile_minima(row_segment, col_segment, row_stats, col_stats, length, barrier, row_start, col_start):
    blocks = (length + COL_BLOCK - 1) // COL_BLOCK

    def add_block(part_index, running):
        row_normal = normalized(row_segment, part_index, row_stats[0], row_stats[1], length).astype(jnp.float32)
        col_normal = normalized(col_segment, part_index, col_stats[0], col_stats[1], length).astype(jnp.float32)
        return running + lax.dot_general(row_normal, col_normal, (((0,), (0,)), ((), ())), precision=lax.Precision.HIGHEST, preferred_element_type=jnp.float32)
    product = lax.fori_loop(0, blocks, add_block, jnp.zeros((TILE_SIDE, TILE_SIDE), jnp.float32))
    distance = 1.0 - product / length.astype(jnp.float32)
    row_ids = row_start + lax.broadcasted_iota(jnp.int32, (TILE_SIDE, 1), 0)
    col_ids = col_start + lax.broadcasted_iota(jnp.int32, (1, TILE_SIDE), 1)
    distance = jnp.where(col_ids - row_ids > barrier, distance, EMPTY_VALUE)
    return (lax.optimization_barrier(jnp.min(distance, axis=1)), lax.optimization_barrier(jnp.min(distance, axis=0)))

def reference(series, window_lengths, exclusion, tile_list):
    positions = TILE_ROWS * TILE_SIDE
    block_ids = jnp.arange(TILE_ROWS, dtype=jnp.int32)

    def one_length(setting):
        length, barrier = setting

        def stats_block(row_block):
            segment = lax.dynamic_slice_in_dim(series, row_block * TILE_SIDE, TILE_SIDE + MAX_LEN)
            return window_stats(segment, length, TILE_SIDE, COL_BLOCK)
        centres, inverses = lax.map(stats_block, block_ids)
        centres = centres.reshape(positions)
        inverses = inverses.reshape(positions)

        def one_tile(profiles, tile_pair):
            right_lowest_distance, left_best = profiles
            row_start = (tile_pair[0] * TILE_SIDE).astype(jnp.int32)
            col_start = (tile_pair[1] * TILE_SIDE).astype(jnp.int32)
            row_segment = lax.dynamic_slice_in_dim(series, row_start, TILE_SIDE + MAX_LEN)
            col_segment = lax.dynamic_slice_in_dim(series, col_start, TILE_SIDE + MAX_LEN)
            row_stats = (lax.dynamic_slice_in_dim(centres, row_start, TILE_SIDE), lax.dynamic_slice_in_dim(inverses, row_start, TILE_SIDE))
            col_stats = (lax.dynamic_slice_in_dim(centres, col_start, TILE_SIDE), lax.dynamic_slice_in_dim(inverses, col_start, TILE_SIDE))
            right_min, left_min = tile_minima(row_segment, col_segment, row_stats, col_stats, length, barrier, row_start, col_start)
            right_old = lax.dynamic_slice_in_dim(right_lowest_distance, row_start, TILE_SIDE)
            right_lowest_distance = lax.dynamic_update_slice_in_dim(right_lowest_distance, jnp.minimum(right_old, right_min), row_start, 0)
            left_old = lax.dynamic_slice_in_dim(left_best, col_start, TILE_SIDE)
            left_best = lax.dynamic_update_slice_in_dim(left_best, jnp.minimum(left_old, left_min), col_start, 0)
            return ((right_lowest_distance, left_best), None)
        blank = jnp.full((positions,), EMPTY_VALUE, jnp.float32)
        profiles, leftover = lax.scan(one_tile, (blank, blank), tile_list)
        return profiles
    right_lowest_distance, left_best = lax.map(one_length, (window_lengths, exclusion))
    return (right_lowest_distance, left_best)
```

```python
import functools

import jax
import jax.numpy as jnp
from jax import lax
from jax.experimental import pallas as pl
from jax.experimental.pallas import tpu as pltpu
from jax.sharding import PartitionSpec as P

MAX_LEN = 1024
TILE_SIDE = 512
LANES = 128
CHUNK = 256

EMPTY_VALUE = 2.0
VAR_EPS = 1e-05

VMEM = pltpu.MemorySpace.VMEM
SMEM = pltpu.MemorySpace.SMEM


def gather_kernel(n, piece_ref, slots_ref, send_sem, recv_sem, own_sem):
    me = lax.axis_index("tile")
    barrier = pltpu.get_barrier_semaphore()

    def greet(step, carry):
        peer = lax.rem(me + step, n)
        pl.semaphore_signal(
            barrier, inc=1, device_id={"tile": peer}, device_id_type=pl.DeviceIdType.MESH
        )
        return carry

    lax.fori_loop(1, n, greet, 0)
    own = pltpu.make_async_copy(piece_ref, slots_ref.at[me], own_sem)
    own.start()
    pl.semaphore_wait(barrier, n - 1)

    def copy(step):
        peer = lax.rem(me + step, n)
        return pltpu.make_async_remote_copy(
            src_ref=piece_ref,
            dst_ref=slots_ref.at[me],
            send_sem=send_sem.at[step],
            recv_sem=recv_sem.at[step],
            device_id={"tile": peer},
            device_id_type=pl.DeviceIdType.MESH,
        )

    def send(step, carry):
        copy(step).start()
        return carry

    def finish(step, carry):
        copy(step).wait()
        return carry

    lax.fori_loop(1, n, send, 0)
    own.wait()
    lax.fori_loop(1, n, finish, 0)


def exchange_kernel(count_len, n, best_ref, parts_ref, send_sem, recv_sem, own_sem):
    total = count_len * n
    my_len = lax.axis_index("len")
    my_tile = lax.axis_index("tile")
    me = my_len * n + my_tile
    barrier = pltpu.get_barrier_semaphore()

    def where(step):
        peer = lax.rem(me + step, total)
        return peer // n, lax.rem(peer, n)

    def greet(step, carry):
        peer_len, peer_tile = where(step)
        pl.semaphore_signal(
            barrier,
            inc=1,
            device_id={"len": peer_len, "tile": peer_tile},
            device_id_type=pl.DeviceIdType.MESH,
        )
        return carry

    lax.fori_loop(1, total, greet, 0)
    own = pltpu.make_async_copy(best_ref.at[my_tile], parts_ref.at[me], own_sem)
    own.start()
    pl.semaphore_wait(barrier, total - 1)

    def copy(step):
        peer_len, peer_tile = where(step)
        return pltpu.make_async_remote_copy(
            src_ref=best_ref.at[peer_tile],
            dst_ref=parts_ref.at[me],
            send_sem=send_sem.at[step],
            recv_sem=recv_sem.at[step],
            device_id={"len": peer_len, "tile": peer_tile},
            device_id_type=pl.DeviceIdType.MESH,
        )

    def send(step, carry):
        copy(step).start()
        return carry

    def finish(step, carry):
        copy(step).wait()
        return carry

    lax.fori_loop(1, total, send, 0)
    own.wait()
    lax.fori_loop(1, total, finish, 0)


def sweep_kernel(
    piece,
    count_len,
    tile_ref,
    length_ref,
    barrier_ref,
    slots_ref,
    best_ref,
    line,
    base,
    full_mean,
    full_spread,
    part_mean,
    part_spread,
    centre_ref,
    inverse_ref,
    left_op,
    right_op,
):
    n = slots_ref.shape[0]
    width = line.shape[1]
    columns = width // LANES
    padded = slots_ref.shape[2]
    blocks = best_ref.shape[0]
    groups = blocks * (TILE_SIDE // LANES)
    reach = MAX_LEN // LANES

    line[...] = jnp.zeros(line.shape, jnp.float32)
    for t in range(n):
        start = t * piece
        low, shift = start // LANES * LANES, start % LANES
        room = min(padded + LANES, width - low)
        row = jnp.concatenate([slots_ref[t], jnp.zeros((1, LANES), jnp.float32)], axis=1)
        if shift:
            row = pltpu.roll(row, shift, 1)
        line[:, low : low + room] += row[:, :room]

    rows8 = jnp.broadcast_to(line[...], (8, width))
    sub = lax.broadcasted_iota(jnp.int32, (8, width), 0)
    for bit in (1, 2, 4):
        rows8 = jnp.where((sub & bit) != 0, pltpu.roll(rows8, width - bit, 1), rows8)
    for g in range(LANES // 8):
        base[8 * g : 8 * g + 8, :] = rows8 if g == 0 else pltpu.roll(rows8, width - 8 * g, 1)

    row_ids = lax.broadcasted_iota(jnp.int32, (LANES, LANES), 0)
    rests = [lax.rem(length_ref[l], LANES) for l in range(count_len)]
    scales = [1.0 / jnp.maximum(rest, 1).astype(jnp.float32) for rest in rests]

    def column_stats(a, carry):
        values = base[:, pl.ds(pl.multiple_of(a * LANES, LANES), LANES)]
        mean = jnp.sum(values, axis=0, keepdims=True) * (1.0 / LANES)
        off = values - mean
        full_mean[pl.ds(a, 1), :] = mean
        full_spread[pl.ds(a, 1), :] = jnp.sum(off * off, axis=0, keepdims=True)
        for l in range(count_len):
            inside = row_ids < rests[l]
            mean = jnp.sum(jnp.where(inside, values, 0.0), axis=0, keepdims=True) * scales[l]
            off = jnp.where(inside, values - mean, 0.0)
            part_mean[l, pl.ds(a, 1), :] = mean
            part_spread[l, pl.ds(a, 1), :] = jnp.sum(off * off, axis=0, keepdims=True)
        return carry

    lax.fori_loop(0, columns, column_stats, 0)

    for l in range(count_len):
        length = length_ref[l]
        size = length.astype(jnp.float32)
        whole = length // LANES
        rest = rests[l].astype(jnp.float32)
        rest_mean = part_mean[l, pl.ds(whole, groups), :]
        total = rest_mean * rest
        for k in range(reach):
            total += jnp.where(k < whole, full_mean[k : k + groups, :] * float(LANES), 0.0)
        centre = total / size
        gap = rest_mean - centre
        spread = part_spread[l, pl.ds(whole, groups), :] + rest * (gap * gap)
        for k in range(reach):
            gap = full_mean[k : k + groups, :] - centre
            spread += jnp.where(
                k < whole, full_spread[k : k + groups, :] + float(LANES) * (gap * gap), 0.0
            )
        centre_ref[l] = centre
        inverse_ref[l] = 1.0 / jnp.sqrt(spread / size + VAR_EPS)

    best_ref[...] = jnp.full(best_ref.shape, EMPTY_VALUE, jnp.float32)
    quarters = TILE_SIDE // LANES
    ratio = CHUNK // LANES

    def one_product(index, carry):
        slot, l = index // count_len, lax.rem(index, count_len)
        row_block, col_block = tile_ref[slot, 0], tile_ref[slot, 1]
        length, barrier = length_ref[l], barrier_ref[l]
        size = length.astype(jnp.float32)
        chunks = (length + CHUNK - 1) // CHUNK
        row_first, col_first = row_block * quarters, col_block * quarters

        stats = jnp.concatenate(
            [centre_ref[l, pl.ds(row_first, quarters), :], inverse_ref[l, pl.ds(row_first, quarters), :]],
            axis=0,
        )
        turned = jnp.transpose(stats)
        row_centre = [jnp.broadcast_to(turned[:, q : q + 1], (LANES, LANES)) for q in range(quarters)]
        row_inverse = [
            jnp.broadcast_to(turned[:, quarters + q : quarters + q + 1], (LANES, LANES))
            for q in range(quarters)
        ]
        lane_ids = lax.broadcasted_iota(jnp.int32, (LANES, LANES), 1)
        col_centre = [centre_ref[l, pl.ds(col_first + u, 1), :] for u in range(quarters)]
        col_inverse = [inverse_ref[l, pl.ds(col_first + u, 1), :] for u in range(quarters)]

        def fill(k, carry):
            here = pl.ds(pl.multiple_of(k * LANES, LANES), LANES)
            inside = lane_ids + k * LANES < length
            for q in range(quarters):
                spot = pl.multiple_of((row_first + q + k) * LANES, LANES)
                values = (base[:, pl.ds(spot, LANES)] - row_centre[q]) * row_inverse[q]
                left_op[q * LANES : (q + 1) * LANES, here] = jnp.where(inside, values, 0.0).astype(
                    jnp.bfloat16
                )
                spot = pl.multiple_of((col_first + q + k) * LANES, LANES)
                values = (base[:, pl.ds(spot, LANES)] - col_centre[q]) * col_inverse[q]
                right_op[here, q * LANES : (q + 1) * LANES] = values.astype(jnp.bfloat16)
            return carry

        lax.fori_loop(0, chunks * ratio, fill, 0)

        def finish(depth):
            product = jnp.dot(
                left_op[:, :depth], right_op[:depth, :], preferred_element_type=jnp.float32
            )
            ahead = (
                lax.broadcasted_iota(jnp.int32, product.shape, 1)
                - lax.broadcasted_iota(jnp.int32, product.shape, 0)
            )
            limit = barrier - (col_block - row_block) * TILE_SIDE
            product = jnp.where(ahead > limit, product, -size)
            col_best = jnp.max(product, axis=0, keepdims=True)
            folded = product[:, :LANES]
            for u in range(1, quarters):
                folded = jnp.maximum(folded, product[:, u * LANES : (u + 1) * LANES])
            row_best = jnp.concatenate(
                [
                    jnp.max(
                        jnp.transpose(folded[q * LANES : (q + 1) * LANES, :]), axis=0, keepdims=True
                    )
                    for q in range(quarters)
                ],
                axis=1,
            )
            spot = (row_block, pl.ds(l, 1))
            best_ref[spot] = jnp.minimum(best_ref[spot], 1.0 - row_best / size)
            spot = (col_block, pl.ds(count_len + l, 1))
            best_ref[spot] = jnp.minimum(best_ref[spot], 1.0 - col_best / size)

        for count in range(1, MAX_LEN // CHUNK + 1):

            @pl.when(chunks == count)
            def _():
                finish(count * CHUNK)

        return carry

    lax.fori_loop(0, tile_ref.shape[0] * count_len, one_product, 0)


def shards(series, window_lengths, exclusion, tile_list):
    n = lax.axis_size("tile")
    len_devices = lax.axis_size("len")
    count_len = window_lengths.shape[0]
    piece = series.shape[0]
    points = piece * n
    positions = points - MAX_LEN
    blocks = positions // TILE_SIDE
    padded = (piece + LANES - 1) // LANES * LANES
    columns = points // LANES
    groups = positions // LANES
    row = jnp.pad(series, (0, padded - piece)).reshape(1, padded)

    slots = pl.pallas_call(
        functools.partial(gather_kernel, n),
        out_shape=jax.ShapeDtypeStruct((n, 1, padded), jnp.float32),
        in_specs=[pl.BlockSpec(memory_space=VMEM)],
        out_specs=pl.BlockSpec(memory_space=VMEM),
        scratch_shapes=[
            pltpu.SemaphoreType.DMA((n,)),
            pltpu.SemaphoreType.DMA((n,)),
            pltpu.SemaphoreType.DMA,
        ],
        compiler_params=pltpu.CompilerParams(collective_id=0, has_side_effects=True),
        name="gather_series",
    )(row)

    best = pl.pallas_call(
        functools.partial(sweep_kernel, piece, count_len),
        out_shape=jax.ShapeDtypeStruct((blocks, 2 * count_len, TILE_SIDE), jnp.float32),
        in_specs=[
            pl.BlockSpec(memory_space=SMEM),
            pl.BlockSpec(memory_space=SMEM),
            pl.BlockSpec(memory_space=SMEM),
            pl.BlockSpec(memory_space=VMEM),
        ],
        out_specs=pl.BlockSpec(memory_space=VMEM),
        scratch_shapes=[
            pltpu.VMEM((1, points), jnp.float32),
            pltpu.VMEM((LANES, points), jnp.float32),
            pltpu.VMEM((columns, LANES), jnp.float32),
            pltpu.VMEM((columns, LANES), jnp.float32),
            pltpu.VMEM((count_len, columns + 8, LANES), jnp.float32),
            pltpu.VMEM((count_len, columns + 8, LANES), jnp.float32),
            pltpu.VMEM((count_len, groups, LANES), jnp.float32),
            pltpu.VMEM((count_len, groups, LANES), jnp.float32),
            pltpu.VMEM((TILE_SIDE, MAX_LEN), jnp.bfloat16),
            pltpu.VMEM((MAX_LEN, TILE_SIDE), jnp.bfloat16),
        ],
        name="sweep_tiles",
    )(tile_list, window_lengths, exclusion, slots)

    total = len_devices * n
    parts = pl.pallas_call(
        functools.partial(exchange_kernel, len_devices, n),
        out_shape=jax.ShapeDtypeStruct((total, 2 * count_len, TILE_SIDE), jnp.float32),
        in_specs=[pl.BlockSpec(memory_space=VMEM)],
        out_specs=pl.BlockSpec(memory_space=VMEM),
        scratch_shapes=[
            pltpu.SemaphoreType.DMA((total,)),
            pltpu.SemaphoreType.DMA((total,)),
            pltpu.SemaphoreType.DMA,
        ],
        compiler_params=pltpu.CompilerParams(collective_id=1, has_side_effects=True),
        name="exchange_minima",
    )(best)
    merged = jnp.min(parts.reshape(len_devices, n, 2, count_len, TILE_SIDE), axis=1)
    right = merged[:, 0].reshape(len_devices * count_len, TILE_SIDE)
    left = merged[:, 1].reshape(len_devices * count_len, TILE_SIDE)
    return (right, left)


def solution(mesh):
    return jax.shard_map(
        shards,
        mesh=mesh,
        in_specs=(P("tile"), P("len"), P("len"), P("tile", None)),
        out_specs=(P(None, "tile"), P(None, "tile")),
        check_vma=False,
    )
```

```python
import functools

import jax
import jax.numpy as jnp
from jax import lax
from jax.experimental import pallas as pl
from jax.experimental.pallas import tpu as pltpu
from jax.sharding import PartitionSpec as P

MAX_LEN = 1024
TILE_SIDE = 512
LANES = 128
CHUNK = 256

EMPTY_VALUE = 2.0
VAR_EPS = 1e-05

VMEM = pltpu.MemorySpace.VMEM
SMEM = pltpu.MemorySpace.SMEM


def signal_all(barrier, axis, n):
    me = lax.axis_index(axis)
    for step in range(1, n):
        pl.semaphore_signal(
            barrier,
            inc=1,
            device_id={axis: lax.rem(me + step, n)},
            device_id_type=pl.DeviceIdType.MESH,
        )


def copy_to(axis, n, step, source, target, send_sem, recv_sem):
    peer = lax.rem(lax.axis_index(axis) + step, n)
    return pltpu.make_async_remote_copy(
        src_ref=source(peer),
        dst_ref=target,
        send_sem=send_sem.at[step],
        recv_sem=recv_sem.at[step],
        device_id={axis: peer},
        device_id_type=pl.DeviceIdType.MESH,
    )


def gather_kernel(n, piece_ref, slots_ref, send_sem, recv_sem, own_sem):
    me = lax.axis_index("tile")
    barrier = pltpu.get_barrier_semaphore()
    signal_all(barrier, "tile", n)
    own = pltpu.make_async_copy(piece_ref, slots_ref.at[me], own_sem)
    own.start()
    pl.semaphore_wait(barrier, n - 1)
    copies = [
        copy_to("tile", n, step, lambda peer: piece_ref, slots_ref.at[me], send_sem, recv_sem)
        for step in range(1, n)
    ]
    for copy in copies:
        copy.start()
    own.wait()
    for copy in copies:
        copy.wait()


def exchange_kernel(
    count_len,
    n,
    best_ref,
    right_ref,
    left_ref,
    parts,
    mine,
    groups,
    send_sem,
    recv_sem,
    own_sem,
    send_len,
    recv_len,
):
    my_len = lax.axis_index("len")
    my_tile = lax.axis_index("tile")
    rows = best_ref.shape[1] // 2
    barrier = pltpu.get_barrier_semaphore()
    signal_all(barrier, "tile", n)
    signal_all(barrier, "len", count_len)
    own = pltpu.make_async_copy(best_ref.at[my_tile], parts.at[my_tile], own_sem)
    own.start()
    pl.semaphore_wait(barrier, n - 1 + count_len - 1)
    copies = [
        copy_to(
            "tile", n, step, lambda peer: best_ref.at[peer], parts.at[my_tile], send_sem, recv_sem
        )
        for step in range(1, n)
    ]
    for copy in copies:
        copy.start()
    own.wait()
    for copy in copies:
        copy.wait_recv()
    merged = jnp.min(parts[...], axis=0)
    mine[...] = merged
    copies_len = [
        copy_to("len", count_len, step, lambda peer: mine, groups.at[my_len], send_len, recv_len)
        for step in range(1, count_len)
    ]
    for copy in copies_len:
        copy.start()
    groups[my_len] = merged
    for copy in copies:
        copy.wait_send()
    for copy in copies_len:
        copy.wait()
    for g in range(count_len):
        right_ref[g * rows : (g + 1) * rows, :] = groups[g, :rows, :]
        left_ref[g * rows : (g + 1) * rows, :] = groups[g, rows:, :]


def shifted(values, count):
    rows = values.shape[0]
    skip, shift = count // LANES, count % LANES
    if shift:
        lane_ids = lax.broadcasted_iota(jnp.int32, values.shape, 1)
        values = pltpu.roll(values, LANES - shift, 1)
        values = jnp.where(lane_ids < LANES - shift, values, pltpu.roll(values, rows - 1, 0))
    if skip:
        values = pltpu.roll(values, rows - skip, 0)
    return values


def window_stats(packed, lengths):
    mean, spread = packed, jnp.zeros_like(packed)
    results = [(jnp.zeros_like(packed), jnp.zeros_like(packed)) for _ in lengths]
    bits = MAX_LEN.bit_length()
    for b in range(bits):
        first = 1 << b
        for l, length in enumerate(lengths):
            tail_mean, tail_spread = results[l]
            if b:
                tail_mean, tail_spread = shifted(tail_mean, first), shifted(tail_spread, first)
            rest = lax.rem(length, first).astype(jnp.float32)
            share = rest / (rest + first)
            gap = tail_mean - mean
            taken = (length & first) != 0
            results[l] = (
                jnp.where(taken, mean + gap * share, results[l][0]),
                jnp.where(
                    taken, spread + tail_spread + gap * gap * (share * first), results[l][1]
                ),
            )
        if b < bits - 1:
            next_mean = shifted(mean, first)
            gap = next_mean - mean
            mean = 0.5 * (mean + next_mean)
            if b:
                spread = spread + shifted(spread, first) + gap * gap * (0.5 * first)
            else:
                spread = gap * gap * 0.5
    return [
        (mean, 1.0 / jnp.sqrt(spread / length.astype(jnp.float32) + VAR_EPS))
        for (mean, spread), length in zip(results, lengths)
    ]


def sweep_kernel(
    piece,
    count_len,
    tile_ref,
    length_ref,
    barrier_ref,
    slots_ref,
    best_ref,
    line,
    base,
    packed,
    centre_ref,
    inverse_ref,
    left_op,
    right_op,
):
    n = slots_ref.shape[0]
    width = line.shape[1]
    columns = width // LANES
    padded = slots_ref.shape[2]

    line[...] = jnp.zeros(line.shape, jnp.float32)
    for t in range(n):
        start = t * piece
        low, shift = start // LANES * LANES, start % LANES
        room = min(padded + LANES, width - low)
        row = jnp.concatenate([slots_ref[t], jnp.zeros((1, LANES), jnp.float32)], axis=1)
        if shift:
            row = pltpu.roll(row, shift, 1)
        line[:, low : low + room] += row[:, :room]
    for a in range(columns):
        packed[a : a + 1, :] = line[:, a * LANES : (a + 1) * LANES]

    lengths = [length_ref[l] for l in range(count_len)]
    for l, (centre, inverse) in enumerate(window_stats(packed[...], lengths)):
        centre_ref[l] = centre
        inverse_ref[l] = inverse

    rows8 = jnp.broadcast_to(line[...], (8, width))
    sub = lax.broadcasted_iota(jnp.int32, (8, width), 0)
    for bit in (1, 2, 4):
        rows8 = jnp.where((sub & bit) != 0, pltpu.roll(rows8, width - bit, 1), rows8)
    for g in range(LANES // 8):
        base[8 * g : 8 * g + 8, :] = rows8 if g == 0 else pltpu.roll(rows8, width - 8 * g, 1)

    best_ref[...] = jnp.full(best_ref.shape, EMPTY_VALUE, jnp.float32)
    quarters = TILE_SIDE // LANES

    def one_product(index, carry):
        slot, l = index // count_len, lax.rem(index, count_len)
        row_block, col_block = tile_ref[slot, 0], tile_ref[slot, 1]
        length, barrier = length_ref[l], barrier_ref[l]
        size = length.astype(jnp.float32)
        chunks = (length + CHUNK - 1) // CHUNK
        row_first, col_first = row_block * quarters, col_block * quarters
        limit = barrier - (col_block - row_block) * TILE_SIDE

        def finish(depth):
            turned = jnp.transpose(
                jnp.concatenate(
                    [
                        centre_ref[l, pl.ds(row_first, quarters), :],
                        inverse_ref[l, pl.ds(row_first, quarters), :],
                    ],
                    axis=0,
                )
            )
            col_centre, col_inverse = (
                jnp.concatenate(
                    [source[l, pl.ds(col_first + u, 1), :] for u in range(quarters)], axis=1
                )
                for source in (centre_ref, inverse_ref)
            )
            for k in range(depth // LANES):
                spot = pl.ds(pl.multiple_of((col_first + k) * LANES, LANES), TILE_SIDE)
                right_op[k * LANES : (k + 1) * LANES, :] = (
                    (base[:, spot] - col_centre) * col_inverse
                ).astype(jnp.bfloat16)
            sure = depth - CHUNK
            lane_ids = lax.broadcasted_iota(jnp.int32, (16, CHUNK), 1)
            inside = lane_ids < length - sure
            col_best = None
            row_best = []
            for half in range(0, quarters, 2):
                for q in range(half, half + 2):
                    spot = pl.ds(pl.multiple_of((row_first + q) * LANES, LANES), depth)
                    for g in range(0, LANES, 16):
                        values = (base[g : g + 16, spot] - turned[g : g + 16, q : q + 1]) * turned[
                            g : g + 16, quarters + q : quarters + q + 1
                        ]
                        last = jnp.where(inside, values[:, sure:], 0.0)
                        at = q * LANES + g
                        if sure:
                            left_op[at : at + 16, :sure] = values[:, :sure].astype(jnp.bfloat16)
                        left_op[at : at + 16, sure:depth] = last.astype(jnp.bfloat16)
                low = half * LANES
                product = jnp.dot(
                    left_op[low : low + 2 * LANES, :depth],
                    right_op[:depth, :],
                    preferred_element_type=jnp.float32,
                )
                ahead = lax.broadcasted_iota(jnp.int32, product.shape, 1) - (
                    lax.broadcasted_iota(jnp.int32, product.shape, 0) + low
                )
                product = jnp.where(ahead > limit, product, -size)
                top = jnp.max(product, axis=0, keepdims=True)
                col_best = top if col_best is None else jnp.maximum(col_best, top)
                folded = product[:, :LANES]
                for u in range(1, quarters):
                    folded = jnp.maximum(folded, product[:, u * LANES : (u + 1) * LANES])
                for q in range(2):
                    turned_back = jnp.transpose(folded[q * LANES : (q + 1) * LANES, :])
                    row_best.append(jnp.max(turned_back, axis=0, keepdims=True))
            row_best = jnp.concatenate(row_best, axis=1)
            spot = (row_block, pl.ds(l, 1))
            best_ref[spot] = jnp.minimum(best_ref[spot], 1.0 - row_best / size)
            spot = (col_block, pl.ds(count_len + l, 1))
            best_ref[spot] = jnp.minimum(best_ref[spot], 1.0 - col_best / size)

        for count in range(1, MAX_LEN // CHUNK + 1):

            @pl.when(chunks == count)
            def _():
                finish(count * CHUNK)

        return carry

    lax.fori_loop(0, tile_ref.shape[0] * count_len, one_product, 0)


def shards(series, window_lengths, exclusion, tile_list):
    n = lax.axis_size("tile")
    len_devices = lax.axis_size("len")
    count_len = window_lengths.shape[0]
    piece = series.shape[0]
    points = piece * n
    positions = points - MAX_LEN
    blocks = positions // TILE_SIDE
    padded = (piece + LANES - 1) // LANES * LANES
    columns = points // LANES
    row = jnp.pad(series, (0, padded - piece)).reshape(1, padded)

    slots = pl.pallas_call(
        functools.partial(gather_kernel, n),
        out_shape=jax.ShapeDtypeStruct((n, 1, padded), jnp.float32),
        in_specs=[pl.BlockSpec(memory_space=VMEM)],
        out_specs=pl.BlockSpec(memory_space=VMEM),
        scratch_shapes=[
            pltpu.SemaphoreType.DMA((n,)),
            pltpu.SemaphoreType.DMA((n,)),
            pltpu.SemaphoreType.DMA,
        ],
        compiler_params=pltpu.CompilerParams(collective_id=0, has_side_effects=True),
        name="gather_series",
    )(row)

    best = pl.pallas_call(
        functools.partial(sweep_kernel, piece, count_len),
        out_shape=jax.ShapeDtypeStruct((blocks, 2 * count_len, TILE_SIDE), jnp.float32),
        in_specs=[
            pl.BlockSpec(memory_space=SMEM),
            pl.BlockSpec(memory_space=SMEM),
            pl.BlockSpec(memory_space=SMEM),
            pl.BlockSpec(memory_space=VMEM),
        ],
        out_specs=pl.BlockSpec(memory_space=VMEM),
        scratch_shapes=[
            pltpu.VMEM((1, points), jnp.float32),
            pltpu.VMEM((LANES, points), jnp.float32),
            pltpu.VMEM((columns, LANES), jnp.float32),
            pltpu.VMEM((count_len, columns, LANES), jnp.float32),
            pltpu.VMEM((count_len, columns, LANES), jnp.float32),
            pltpu.VMEM((TILE_SIDE, MAX_LEN), jnp.bfloat16),
            pltpu.VMEM((MAX_LEN, TILE_SIDE), jnp.bfloat16),
        ],
        name="sweep_tiles",
    )(tile_list, window_lengths, exclusion, slots)

    block = (2 * count_len, TILE_SIDE)
    profile = jax.ShapeDtypeStruct((len_devices * count_len, TILE_SIDE), jnp.float32)
    return pl.pallas_call(
        functools.partial(exchange_kernel, len_devices, n),
        out_shape=(profile, profile),
        in_specs=[pl.BlockSpec(memory_space=VMEM)],
        out_specs=(pl.BlockSpec(memory_space=VMEM), pl.BlockSpec(memory_space=VMEM)),
        scratch_shapes=[
            pltpu.VMEM((n, *block), jnp.float32),
            pltpu.VMEM(block, jnp.float32),
            pltpu.VMEM((len_devices, *block), jnp.float32),
            pltpu.SemaphoreType.DMA((n,)),
            pltpu.SemaphoreType.DMA((n,)),
            pltpu.SemaphoreType.DMA,
            pltpu.SemaphoreType.DMA((len_devices,)),
            pltpu.SemaphoreType.DMA((len_devices,)),
        ],
        compiler_params=pltpu.CompilerParams(collective_id=1, has_side_effects=True),
        name="exchange_minima",
    )(best)


def solution(mesh):
    return jax.shard_map(
        shards,
        mesh=mesh,
        in_specs=(P("tile"), P("len"), P("len"), P("tile", None)),
        out_specs=(P(None, "tile"), P(None, "tile")),
        check_vma=False,
    )
```

```python
import functools

import jax
import jax.numpy as jnp
from jax import lax
from jax.experimental import pallas as pl
from jax.experimental.pallas import tpu as pltpu
from jax.sharding import PartitionSpec as P

MAX_LEN = 1024
TILE_SIDE = 512
LANES = 128
CHUNK = 256
GRANT = 1 << 20
FLAT = 1024

EMPTY_VALUE = 2.0
VAR_EPS = 1e-05

VMEM = pltpu.MemorySpace.VMEM
SMEM = pltpu.MemorySpace.SMEM


def signal_all(barrier, axis, n):
    me = lax.axis_index(axis)
    for step in range(1, n):
        pl.semaphore_signal(
            barrier,
            inc=1,
            device_id={axis: lax.rem(me + step, n)},
            device_id_type=pl.DeviceIdType.MESH,
        )


def copy_to(axis, n, step, source, target, send_sem, recv_sem):
    peer = lax.rem(lax.axis_index(axis) + step, n)
    return pltpu.make_async_remote_copy(
        src_ref=source(peer),
        dst_ref=target,
        send_sem=send_sem.at[step],
        recv_sem=recv_sem.at[step],
        device_id={axis: peer},
        device_id_type=pl.DeviceIdType.MESH,
    )


def gather_kernel(n, piece_ref, slots_ref, staged, send_sem, recv_sem, own_sem):
    me = lax.axis_index("tile")
    stride = slots_ref.shape[0] // n
    slot = slots_ref.at[pl.ds(pl.multiple_of(me * stride, FLAT), staged.shape[0])]
    staged[...] = jnp.zeros(staged.shape, jnp.float32)
    staged[: piece_ref.shape[0]] = piece_ref[...]
    barrier = pltpu.get_barrier_semaphore()
    signal_all(barrier, "tile", n)
    own = pltpu.make_async_copy(staged, slot, own_sem)
    own.start()
    pl.semaphore_wait(barrier, n - 1)
    copies = [
        copy_to("tile", n, step, lambda peer: staged, slot, send_sem, recv_sem)
        for step in range(1, n)
    ]
    for copy in copies:
        copy.start()
    own.wait()
    for copy in copies:
        copy.wait()


def exchange_kernel(
    count_len,
    n,
    best_ref,
    right_ref,
    left_ref,
    parts,
    mine,
    groups,
    send_sem,
    recv_sem,
    own_sem,
    send_len,
    recv_len,
):
    my_len = lax.axis_index("len")
    my_tile = lax.axis_index("tile")
    rows = best_ref.shape[1] // 2
    barrier = pltpu.get_barrier_semaphore()
    signal_all(barrier, "tile", n)
    signal_all(barrier, "len", count_len)
    own = pltpu.make_async_copy(best_ref.at[my_tile], parts.at[my_tile], own_sem)
    own.start()
    pl.semaphore_wait(barrier, n - 1 + count_len - 1)
    copies = [
        copy_to(
            "tile", n, step, lambda peer: best_ref.at[peer], parts.at[my_tile], send_sem, recv_sem
        )
        for step in range(1, n)
    ]
    for copy in copies:
        copy.start()
    own.wait()
    for copy in copies:
        copy.wait_recv()
    merged = jnp.min(parts[...], axis=0)
    mine[...] = merged
    copies_len = [
        copy_to("len", count_len, step, lambda peer: mine, groups.at[my_len], send_len, recv_len)
        for step in range(1, count_len)
    ]
    for copy in copies_len:
        copy.start()
    groups[my_len] = merged
    for copy in copies:
        copy.wait_send()
    for copy in copies_len:
        copy.wait()
    for g in range(count_len):
        right_ref[g * rows : (g + 1) * rows, :] = groups[g, :rows, :]
        left_ref[g * rows : (g + 1) * rows, :] = groups[g, rows:, :]


def shifted(values, count):
    rows = values.shape[0]
    skip, shift = count // LANES, count % LANES
    if shift:
        lane_ids = lax.broadcasted_iota(jnp.int32, values.shape, 1)
        values = pltpu.roll(values, LANES - shift, 1)
        values = jnp.where(lane_ids < LANES - shift, values, pltpu.roll(values, rows - 1, 0))
    if skip:
        values = pltpu.roll(values, rows - skip, 0)
    return values


def window_stats(packed, lengths):
    mean, spread = packed, jnp.zeros_like(packed)
    results = [(jnp.zeros_like(packed), jnp.zeros_like(packed)) for _ in lengths]
    bits = MAX_LEN.bit_length()
    for b in range(bits):
        first = 1 << b
        for l, length in enumerate(lengths):
            tail_mean, tail_spread = results[l]
            if b:
                tail_mean, tail_spread = shifted(tail_mean, first), shifted(tail_spread, first)
            rest = lax.rem(length, first).astype(jnp.float32)
            share = rest / (rest + first)
            gap = tail_mean - mean
            taken = (length & first) != 0
            results[l] = (
                jnp.where(taken, mean + gap * share, results[l][0]),
                jnp.where(
                    taken, spread + tail_spread + gap * gap * (share * first), results[l][1]
                ),
            )
        if b < bits - 1:
            next_mean = shifted(mean, first)
            gap = next_mean - mean
            mean = 0.5 * (mean + next_mean)
            if b:
                spread = spread + shifted(spread, first) + gap * gap * (0.5 * first)
            else:
                spread = gap * gap * 0.5
    return [
        (mean, 1.0 / jnp.sqrt(spread / length.astype(jnp.float32) + VAR_EPS))
        for (mean, spread), length in zip(results, lengths)
    ]


def sweep_kernel(
    piece,
    count_len,
    tile_ref,
    length_ref,
    barrier_ref,
    slots_ref,
    best_ref,
    line,
    base,
    packed,
    centre_ref,
    inverse_ref,
    left_op,
    right_op,
):
    width = line.shape[1]
    columns = width // LANES
    n = width // piece
    stride = slots_ref.shape[0] // n
    padded = (piece + LANES - 1) // LANES * LANES

    line[...] = jnp.zeros(line.shape, jnp.float32)
    for t in range(n):
        start = t * piece
        low, shift = start // LANES * LANES, start % LANES
        room = min(padded + LANES, width - low)
        row = slots_ref[t * stride : t * stride + padded].reshape(1, padded)
        row = jnp.concatenate([row, jnp.zeros((1, LANES), jnp.float32)], axis=1)
        if shift:
            row = pltpu.roll(row, shift, 1)
        line[:, low : low + room] += row[:, :room]
    for a in range(columns):
        packed[a : a + 1, :] = line[:, a * LANES : (a + 1) * LANES]

    lengths = [length_ref[l] for l in range(count_len)]
    for l, (centre, inverse) in enumerate(window_stats(packed[...], lengths)):
        centre_ref[l] = centre
        inverse_ref[l] = inverse

    rows8 = jnp.broadcast_to(line[...], (8, width))
    sub = lax.broadcasted_iota(jnp.int32, (8, width), 0)
    for bit in (1, 2, 4):
        rows8 = jnp.where((sub & bit) != 0, pltpu.roll(rows8, width - bit, 1), rows8)
    for g in range(LANES // 8):
        base[8 * g : 8 * g + 8, :] = rows8 if g == 0 else pltpu.roll(rows8, width - 8 * g, 1)

    best_ref[...] = jnp.full(best_ref.shape, EMPTY_VALUE, jnp.float32)
    quarters = TILE_SIDE // LANES

    def one_product(index, carry):
        slot, l = index // count_len, lax.rem(index, count_len)
        row_block, col_block = tile_ref[0, slot], tile_ref[1, slot]
        length, barrier = length_ref[l], barrier_ref[l]
        size = length.astype(jnp.float32)
        chunks = (length + CHUNK - 1) // CHUNK
        row_first, col_first = row_block * quarters, col_block * quarters
        limit = barrier - (col_block - row_block) * TILE_SIDE

        def finish(depth):
            turned = jnp.transpose(
                jnp.concatenate(
                    [
                        centre_ref[l, pl.ds(row_first, quarters), :],
                        inverse_ref[l, pl.ds(row_first, quarters), :],
                    ],
                    axis=0,
                )
            )
            col_centre, col_inverse = (
                jnp.concatenate(
                    [source[l, pl.ds(col_first + u, 1), :] for u in range(quarters)], axis=1
                )
                for source in (centre_ref, inverse_ref)
            )
            for k in range(depth // LANES):
                spot = pl.ds(pl.multiple_of((col_first + k) * LANES, LANES), TILE_SIDE)
                right_op[k * LANES : (k + 1) * LANES, :] = (
                    (base[:, spot] - col_centre) * col_inverse
                ).astype(jnp.bfloat16)
            sure = depth - CHUNK
            lane_ids = lax.broadcasted_iota(jnp.int32, (16, CHUNK), 1)
            inside = lane_ids < length - sure
            col_best = None
            row_best = []
            for half in range(0, quarters, 2):
                for q in range(half, half + 2):
                    spot = pl.ds(pl.multiple_of((row_first + q) * LANES, LANES), depth)
                    for g in range(0, LANES, 16):
                        values = (base[g : g + 16, spot] - turned[g : g + 16, q : q + 1]) * turned[
                            g : g + 16, quarters + q : quarters + q + 1
                        ]
                        last = jnp.where(inside, values[:, sure:], 0.0)
                        at = q * LANES + g
                        if sure:
                            left_op[at : at + 16, :sure] = values[:, :sure].astype(jnp.bfloat16)
                        left_op[at : at + 16, sure:depth] = last.astype(jnp.bfloat16)
                low = half * LANES
                product = jnp.dot(
                    left_op[low : low + 2 * LANES, :depth],
                    right_op[:depth, :],
                    preferred_element_type=jnp.float32,
                )
                ahead = lax.broadcasted_iota(jnp.int32, product.shape, 1) - (
                    lax.broadcasted_iota(jnp.int32, product.shape, 0) + low
                )
                product = jnp.where(ahead > limit, product, -size)
                top = jnp.max(product, axis=0, keepdims=True)
                col_best = top if col_best is None else jnp.maximum(col_best, top)
                folded = product[:, :LANES]
                for u in range(1, quarters):
                    folded = jnp.maximum(folded, product[:, u * LANES : (u + 1) * LANES])
                for q in range(2):
                    turned_back = jnp.transpose(folded[q * LANES : (q + 1) * LANES, :])
                    row_best.append(jnp.max(turned_back, axis=0, keepdims=True))
            row_best = jnp.concatenate(row_best, axis=1)
            spot = (row_block, pl.ds(l, 1))
            best_ref[spot] = jnp.minimum(best_ref[spot], 1.0 - row_best / size)
            spot = (col_block, pl.ds(count_len + l, 1))
            best_ref[spot] = jnp.minimum(best_ref[spot], 1.0 - col_best / size)

        for count in range(1, MAX_LEN // CHUNK + 1):

            @pl.when(chunks == count)
            def _():
                finish(count * CHUNK)

        return carry

    lax.fori_loop(0, tile_ref.shape[1] * count_len, one_product, 0)


def shards(series, window_lengths, exclusion, tile_list):
    n = lax.axis_size("tile")
    len_devices = lax.axis_size("len")
    count_len = window_lengths.shape[0]
    piece = series.shape[0]
    points = piece * n
    positions = points - MAX_LEN
    blocks = positions // TILE_SIDE
    stride = (piece + FLAT - 1) // FLAT * FLAT
    columns = points // LANES

    slots = pl.pallas_call(
        functools.partial(gather_kernel, n),
        out_shape=jax.ShapeDtypeStruct((n * stride,), jnp.float32),
        in_specs=[pl.BlockSpec(memory_space=VMEM)],
        out_specs=pl.BlockSpec(memory_space=VMEM),
        scratch_shapes=[
            pltpu.VMEM(((piece + LANES - 1) // LANES * LANES,), jnp.float32),
            pltpu.SemaphoreType.DMA((n,)),
            pltpu.SemaphoreType.DMA((n,)),
            pltpu.SemaphoreType.DMA,
        ],
        compiler_params=pltpu.CompilerParams(
            collective_id=0, has_side_effects=True, vmem_limit_bytes=GRANT
        ),
        name="gather_series",
    )(series)

    best = pl.pallas_call(
        functools.partial(sweep_kernel, piece, count_len),
        out_shape=jax.ShapeDtypeStruct((blocks, 2 * count_len, TILE_SIDE), jnp.float32),
        in_specs=[
            pl.BlockSpec(memory_space=SMEM),
            pl.BlockSpec(memory_space=SMEM),
            pl.BlockSpec(memory_space=SMEM),
            pl.BlockSpec(memory_space=VMEM),
        ],
        out_specs=pl.BlockSpec(memory_space=VMEM),
        scratch_shapes=[
            pltpu.VMEM((1, points), jnp.float32),
            pltpu.VMEM((LANES, points), jnp.float32),
            pltpu.VMEM((columns, LANES), jnp.float32),
            pltpu.VMEM((count_len, columns, LANES), jnp.float32),
            pltpu.VMEM((count_len, columns, LANES), jnp.float32),
            pltpu.VMEM((TILE_SIDE, MAX_LEN), jnp.bfloat16),
            pltpu.VMEM((MAX_LEN, TILE_SIDE), jnp.bfloat16),
        ],
        compiler_params=pltpu.CompilerParams(vmem_limit_bytes=32 * GRANT // 2 + points * LANES * 4),
        name="sweep_tiles",
    )(tile_list.T, window_lengths, exclusion, slots)

    block = (2 * count_len, TILE_SIDE)
    profile = jax.ShapeDtypeStruct((len_devices * count_len, TILE_SIDE), jnp.float32)
    return pl.pallas_call(
        functools.partial(exchange_kernel, len_devices, n),
        out_shape=(profile, profile),
        in_specs=[pl.BlockSpec(memory_space=VMEM)],
        out_specs=(pl.BlockSpec(memory_space=VMEM), pl.BlockSpec(memory_space=VMEM)),
        scratch_shapes=[
            pltpu.VMEM((n, *block), jnp.float32),
            pltpu.VMEM(block, jnp.float32),
            pltpu.VMEM((len_devices, *block), jnp.float32),
            pltpu.SemaphoreType.DMA((n,)),
            pltpu.SemaphoreType.DMA((n,)),
            pltpu.SemaphoreType.DMA,
            pltpu.SemaphoreType.DMA((len_devices,)),
            pltpu.SemaphoreType.DMA((len_devices,)),
        ],
        compiler_params=pltpu.CompilerParams(
            collective_id=1, has_side_effects=True, vmem_limit_bytes=2 * GRANT
        ),
        name="exchange_minima",
    )(best)


def solution(mesh):
    return jax.shard_map(
        shards,
        mesh=mesh,
        in_specs=(P("tile"), P("len"), P("len"), P("tile", None)),
        out_specs=(P(None, "tile"), P(None, "tile")),
        check_vma=False,
    )
```

```python
import functools
import itertools

import jax
import jax.numpy as jnp
from jax import lax
from jax.experimental import pallas as pl
from jax.experimental.pallas import tpu as pltpu
from jax.sharding import PartitionSpec as P

MAX_LEN = 1024
TILE_SIDE = 512
LANES = 128
GRANT = 1 << 20
FLAT = 1024

EMPTY_VALUE = 2.0
VAR_EPS = 1e-05

VMEM = pltpu.MemorySpace.VMEM
SMEM = pltpu.MemorySpace.SMEM


def signal_all(barrier, axis, n):
    me = lax.axis_index(axis)
    for step in range(1, n):
        pl.semaphore_signal(
            barrier,
            inc=1,
            device_id={axis: lax.rem(me + step, n)},
            device_id_type=pl.DeviceIdType.MESH,
        )


def copy_to(axis, n, step, source, target, send_sem, recv_sem):
    peer = lax.rem(lax.axis_index(axis) + step, n)
    return pltpu.make_async_remote_copy(
        src_ref=source(peer),
        dst_ref=target,
        send_sem=send_sem.at[step],
        recv_sem=recv_sem.at[step],
        device_id={axis: peer},
        device_id_type=pl.DeviceIdType.MESH,
    )


def gather_kernel(n, piece_ref, slots_ref, staged, send_sem, recv_sem, own_sem):
    me = lax.axis_index("tile")
    stride = slots_ref.shape[0] // n
    slot = slots_ref.at[pl.ds(pl.multiple_of(me * stride, FLAT), staged.shape[0])]
    staged[...] = jnp.zeros(staged.shape, jnp.float32)
    staged[: piece_ref.shape[0]] = piece_ref[...]
    barrier = pltpu.get_barrier_semaphore()
    signal_all(barrier, "tile", n)
    own = pltpu.make_async_copy(staged, slot, own_sem)
    own.start()
    pl.semaphore_wait(barrier, n - 1)
    copies = [
        copy_to("tile", n, step, lambda peer: staged, slot, send_sem, recv_sem)
        for step in range(1, n)
    ]
    for copy in copies:
        copy.start()
    own.wait()
    for copy in copies:
        copy.wait()


def exchange_kernel(
    count_len,
    n,
    best_ref,
    right_ref,
    left_ref,
    parts,
    mine,
    groups,
    send_sem,
    recv_sem,
    own_sem,
    send_len,
    recv_len,
):
    my_len = lax.axis_index("len")
    my_tile = lax.axis_index("tile")
    rows = best_ref.shape[1] // 2
    barrier = pltpu.get_barrier_semaphore()
    signal_all(barrier, "tile", n)
    signal_all(barrier, "len", count_len)
    own = pltpu.make_async_copy(best_ref.at[my_tile], parts.at[my_tile], own_sem)
    own.start()
    pl.semaphore_wait(barrier, n - 1 + count_len - 1)
    copies = [
        copy_to(
            "tile", n, step, lambda peer: best_ref.at[peer], parts.at[my_tile], send_sem, recv_sem
        )
        for step in range(1, n)
    ]
    for copy in copies:
        copy.start()
    own.wait()
    for copy in copies:
        copy.wait_recv()
    merged = jnp.min(parts[...], axis=0)
    mine[...] = merged
    copies_len = [
        copy_to("len", count_len, step, lambda peer: mine, groups.at[my_len], send_len, recv_len)
        for step in range(1, count_len)
    ]
    for copy in copies_len:
        copy.start()
    groups[my_len] = merged
    for copy in copies:
        copy.wait_send()
    for copy in copies_len:
        copy.wait()
    for g in range(count_len):
        right_ref[g * rows : (g + 1) * rows, :] = groups[g, :rows, :]
        left_ref[g * rows : (g + 1) * rows, :] = groups[g, rows:, :]


def shifted(values, count):
    rows = values.shape[0]
    skip, shift = count // LANES, count % LANES
    if shift:
        lane_ids = lax.broadcasted_iota(jnp.int32, values.shape, 1)
        values = pltpu.roll(values, LANES - shift, 1)
        values = jnp.where(lane_ids < LANES - shift, values, pltpu.roll(values, rows - 1, 0))
    if skip:
        values = pltpu.roll(values, rows - skip, 0)
    return values


def window_stats(packed, lengths):
    mean, spread = packed, jnp.zeros_like(packed)
    results = [(jnp.zeros_like(packed), jnp.zeros_like(packed)) for _ in lengths]
    bits = MAX_LEN.bit_length()
    for b in range(bits):
        first = 1 << b
        for l, length in enumerate(lengths):
            tail_mean, tail_spread = results[l]
            if b:
                tail_mean, tail_spread = shifted(tail_mean, first), shifted(tail_spread, first)
            rest = lax.rem(length, first).astype(jnp.float32)
            share = rest / (rest + first)
            gap = tail_mean - mean
            taken = (length & first) != 0
            results[l] = (
                jnp.where(taken, mean + gap * share, results[l][0]),
                jnp.where(
                    taken, spread + tail_spread + gap * gap * (share * first), results[l][1]
                ),
            )
        if b < bits - 1:
            next_mean = shifted(mean, first)
            gap = next_mean - mean
            mean = 0.5 * (mean + next_mean)
            if b:
                spread = spread + shifted(spread, first) + gap * gap * (0.5 * first)
            else:
                spread = gap * gap * 0.5
    return [
        (mean, 1.0 / jnp.sqrt(spread / length.astype(jnp.float32) + VAR_EPS))
        for (mean, spread), length in zip(results, lengths)
    ]


def sweep_kernel(
    piece,
    count_len,
    tile_ref,
    length_ref,
    barrier_ref,
    slots_ref,
    best_ref,
    line,
    base,
    packed,
    centre_ref,
    inverse_ref,
    left_op,
    right_op,
):
    width = line.shape[1]
    columns = width // LANES
    n = width // piece
    stride = slots_ref.shape[0] // n
    padded = (piece + LANES - 1) // LANES * LANES

    line[...] = jnp.zeros(line.shape, jnp.float32)
    for t in range(n):
        start = t * piece
        low, shift = start // LANES * LANES, start % LANES
        room = min(padded + LANES, width - low)
        row = slots_ref[t * stride : t * stride + padded].reshape(1, padded)
        row = jnp.concatenate([row, jnp.zeros((1, LANES), jnp.float32)], axis=1)
        if shift:
            row = pltpu.roll(row, shift, 1)
        line[:, low : low + room] += row[:, :room]
    for a in range(columns):
        packed[a : a + 1, :] = line[:, a * LANES : (a + 1) * LANES]

    lengths = [length_ref[l] for l in range(count_len)]
    for l, (centre, inverse) in enumerate(window_stats(packed[...], lengths)):
        centre_ref[l] = centre
        inverse_ref[l] = inverse

    rows8 = jnp.broadcast_to(line[...], (8, width))
    sub = lax.broadcasted_iota(jnp.int32, (8, width), 0)
    for bit in (1, 2, 4):
        rows8 = jnp.where((sub & bit) != 0, pltpu.roll(rows8, width - bit, 1), rows8)
    for g in range(LANES // 8):
        base[8 * g : 8 * g + 8, :] = rows8 if g == 0 else pltpu.roll(rows8, width - 8 * g, 1)

    best_ref[...] = jnp.full(best_ref.shape, EMPTY_VALUE, jnp.float32)
    quarters = TILE_SIDE // LANES

    def one_product(slot, l, depth):
        row_block, col_block = tile_ref[0, slot], tile_ref[1, slot]
        length, barrier = length_ref[l], barrier_ref[l]
        size = length.astype(jnp.float32)
        row_first, col_first = row_block * quarters, col_block * quarters
        limit = barrier - (col_block - row_block) * TILE_SIDE

        def finish(depth):
            row_centre, row_inverse, col_centre, col_inverse = (
                jnp.concatenate(
                    [source[l, pl.ds(start + u, 1), :] for u in range(quarters)], axis=1
                )
                for start in (row_first, col_first)
                for source in (centre_ref, inverse_ref)
            )
            for k in range(depth // LANES):
                spot = pl.ds(pl.multiple_of((col_first + k) * LANES, LANES), TILE_SIDE)
                right_op[l, k * LANES : (k + 1) * LANES, :] = (
                    (base[:, spot] - col_centre) * col_inverse
                ).astype(jnp.bfloat16)
            for k in range(depth // LANES):
                inside = lax.broadcasted_iota(jnp.int32, (LANES, TILE_SIDE), 0) < length - k * LANES
                spot = pl.ds(pl.multiple_of((row_first + k) * LANES, LANES), TILE_SIDE)
                left_op[l, k * LANES : (k + 1) * LANES, :] = jnp.where(
                    inside, (base[:, spot] - row_centre) * row_inverse, 0.0
                ).astype(jnp.bfloat16)
            col_best = None
            row_best = []
            for half in range(0, quarters, 2):
                low = half * LANES
                product = lax.dot_general(
                    left_op[l, :depth, low : low + 2 * LANES],
                    right_op[l, :depth, :],
                    (((0,), (0,)), ((), ())),
                    preferred_element_type=jnp.float32,
                )
                ahead = lax.broadcasted_iota(jnp.int32, product.shape, 1) - (
                    lax.broadcasted_iota(jnp.int32, product.shape, 0) + low
                )
                product = jnp.where(ahead > limit, product, -size)
                top = jnp.max(product, axis=0, keepdims=True)
                col_best = top if col_best is None else jnp.maximum(col_best, top)
                folded = product[:, :LANES]
                for u in range(1, quarters):
                    folded = jnp.maximum(folded, product[:, u * LANES : (u + 1) * LANES])
                for q in range(2):
                    turned_back = jnp.transpose(folded[q * LANES : (q + 1) * LANES, :])
                    row_best.append(jnp.max(turned_back, axis=0, keepdims=True))
            row_best = jnp.concatenate(row_best, axis=1)
            spot = (row_block, pl.ds(l, 1))
            best_ref[spot] = jnp.minimum(best_ref[spot], 1.0 - row_best / size)
            spot = (col_block, pl.ds(count_len + l, 1))
            best_ref[spot] = jnp.minimum(best_ref[spot], 1.0 - col_best / size)

        finish(depth)

    def one_slot(slot, carry):
        for depths in itertools.product((MAX_LEN // 2, MAX_LEN), repeat=count_len):
            fits = [
                jnp.logical_and(length_ref[l] <= depth, length_ref[l] > depth - MAX_LEN // 2)
                for l, depth in enumerate(depths)
            ]

            @pl.when(functools.reduce(jnp.logical_and, fits))
            def _():
                for l, depth in enumerate(depths):
                    one_product(slot, l, depth)

        return carry

    lax.fori_loop(0, tile_ref.shape[1], one_slot, 0)


def shards(series, window_lengths, exclusion, tile_list):
    n = lax.axis_size("tile")
    len_devices = lax.axis_size("len")
    count_len = window_lengths.shape[0]
    piece = series.shape[0]
    points = piece * n
    positions = points - MAX_LEN
    blocks = positions // TILE_SIDE
    stride = (piece + FLAT - 1) // FLAT * FLAT
    columns = points // LANES

    slots = pl.pallas_call(
        functools.partial(gather_kernel, n),
        out_shape=jax.ShapeDtypeStruct((n * stride,), jnp.float32),
        in_specs=[pl.BlockSpec(memory_space=VMEM)],
        out_specs=pl.BlockSpec(memory_space=VMEM),
        scratch_shapes=[
            pltpu.VMEM(((piece + LANES - 1) // LANES * LANES,), jnp.float32),
            pltpu.SemaphoreType.DMA((n,)),
            pltpu.SemaphoreType.DMA((n,)),
            pltpu.SemaphoreType.DMA,
        ],
        compiler_params=pltpu.CompilerParams(
            collective_id=0, has_side_effects=True, vmem_limit_bytes=GRANT
        ),
        name="gather_series",
    )(series)

    best = pl.pallas_call(
        functools.partial(sweep_kernel, piece, count_len),
        out_shape=jax.ShapeDtypeStruct((blocks, 2 * count_len, TILE_SIDE), jnp.float32),
        in_specs=[
            pl.BlockSpec(memory_space=SMEM),
            pl.BlockSpec(memory_space=SMEM),
            pl.BlockSpec(memory_space=SMEM),
            pl.BlockSpec(memory_space=VMEM),
        ],
        out_specs=pl.BlockSpec(memory_space=VMEM),
        scratch_shapes=[
            pltpu.VMEM((1, points), jnp.float32),
            pltpu.VMEM((LANES, points), jnp.float32),
            pltpu.VMEM((columns, LANES), jnp.float32),
            pltpu.VMEM((count_len, columns, LANES), jnp.float32),
            pltpu.VMEM((count_len, columns, LANES), jnp.float32),
            pltpu.VMEM((count_len, MAX_LEN, TILE_SIDE), jnp.bfloat16),
            pltpu.VMEM((count_len, MAX_LEN, TILE_SIDE), jnp.bfloat16),
        ],
        compiler_params=pltpu.CompilerParams(vmem_limit_bytes=32 * GRANT // 2 + points * LANES * 4),
        name="sweep_tiles",
    )(tile_list.T, window_lengths, exclusion, slots)

    block = (2 * count_len, TILE_SIDE)
    profile = jax.ShapeDtypeStruct((len_devices * count_len, TILE_SIDE), jnp.float32)
    return pl.pallas_call(
        functools.partial(exchange_kernel, len_devices, n),
        out_shape=(profile, profile),
        in_specs=[pl.BlockSpec(memory_space=VMEM)],
        out_specs=(pl.BlockSpec(memory_space=VMEM), pl.BlockSpec(memory_space=VMEM)),
        scratch_shapes=[
            pltpu.VMEM((n, *block), jnp.float32),
            pltpu.VMEM(block, jnp.float32),
            pltpu.VMEM((len_devices, *block), jnp.float32),
            pltpu.SemaphoreType.DMA((n,)),
            pltpu.SemaphoreType.DMA((n,)),
            pltpu.SemaphoreType.DMA,
            pltpu.SemaphoreType.DMA((len_devices,)),
            pltpu.SemaphoreType.DMA((len_devices,)),
        ],
        compiler_params=pltpu.CompilerParams(
            collective_id=1, has_side_effects=True, vmem_limit_bytes=2 * GRANT
        ),
        name="exchange_minima",
    )(best)


def solution(mesh):
    return jax.shard_map(
        shards,
        mesh=mesh,
        in_specs=(P("tile"), P("len"), P("len"), P("tile", None)),
        out_specs=(P(None, "tile"), P(None, "tile")),
        check_vma=False,
    )
```
